32 devices in a mesh: dp: 16 (over z, y, core), mp: 2 (over x).
Axes of the slice: x: 2, y: 2, z: 4, core: 2. Of those that a mesh axis runs over, the one named last changes fastest.
Arguments:
- bag_lengths: int32 [16, 2048], P('mp', 'dp'), may hold values from 1 to 8
- owners: int32 [16, 2048, 8, 1], P('mp', 'dp'), may hold values from 0 to 15; in each aligned block of 1024 rows (0 to 1023, 1024 to 2047, ..., all dimensions but the last counted through in order) at most 128 rows name the same one
- row_slots: int32 [16, 2048, 8], P('mp', 'dp'), may hold values from 0 to 511
- admit_mask: int32 [16, 2048, 8], P('mp', 'dp'), may hold values 0 or 1
- expired: int32 [16, 8192], P('mp', 'dp'), may hold values 0 or 1
- embeddings: float32 [16, 8192, 128], P('mp', 'dp'), may hold values from -3 to 3
- accumulator: float32 [16, 8192], P('mp', 'dp'), may hold values from 0.001 to 0.01
- hidden_weight: bfloat16 [2048, 1024], P(None, 'mp'), may hold values from -0.125 to 0.125
- output_weight: float32 [1024], P('mp'), may hold values from -0.9 to 0.9
- labels: int32 [2048], P('dp'), may hold values 0 or 1
Outputs:
- new_table: float32 [16, 8192, 128], P('mp', 'dp')
- new_accum: float32 [16, 8192], P('mp', 'dp')
- weight_grad: bfloat16 [2048, 1024], P(None, 'mp')
- logits: float32 [2048], P('dp')
The draws below stay inside these ranges and needn't reach their ends.
Inputs may be any that keep to these rules, and one draw needn't show every extreme that they name: Among the 128 x 8 lookups of one index of dp into one table (aligned blocks of owners' rows), at most 128 name the same owner; in some blocks one owner is named exactly 128 times.
All inputs are finite; a program needn't handle non-finite values. No bound on the sum of `admit_mask` or of `expired` or of `labels` on one device may be relied on, other than what follows from the above.
Results may differ from the reference program's by a relative error of at most 0.0085.
Values may be sent and summed in bfloat16 or wider, within the bound.
A program may use at most 64 MiB of HBM per device.

```python
import math
import jax
import jax.numpy as jnp
import numpy as np
from jax import lax

TABLES = 16
EMB = 128
HIDDEN_SIZE = 1024
BAG = 8
ROWS_DEV = 512
TOK_DEV = 128
TOKENS = 2048
ROWS = 8192
CAP = 128
N_DP = 16


def set_ends(array, key, least, high):
    longest = array.shape.index(max(array.shape))
    spots = []
    for shift in (0, 1):
        where = [jax.random.randint(jax.random.fold_in(key, axis), (), 0, length) for axis, length in enumerate(array.shape)]
        where[longest] = (where[longest] + shift) % array.shape[longest]
        spots.append(tuple(where))
    return array.at[spots[0]].set(least).at[spots[1]].set(high)


def level_of(key, extent, cuts, smallest, top_value):
    gain, own = 1.0, jax.random.fold_in(key, 6)
    for dim, blocks in cuts:
        steps = jnp.exp(jax.random.uniform(jax.random.fold_in(own, dim), (blocks,), jnp.float32, smallest / len(cuts), top_value / len(cuts)))
        gain = gain * jnp.repeat(steps, extent[dim] // blocks).reshape([-1 if axis == dim else 1 for axis in range(len(extent))])
    return gain


def rank_table(count, skew):
    portions = [(1 << 20) // math.isqrt(rank ** skew) + 1 for rank in range(1, count + 1)]
    spread = 1 + sum(portions) // (1 << 30)
    return np.cumsum(np.array([max(1, weight // spread) for weight in portions]))


def skewed_ids(stream_key, extent, number_of, slope):
    table = rank_table(number_of, slope)
    ticket = jax.random.randint(jax.random.fold_in(stream_key, 1), extent, 0, int(table[number_of - 1]))
    rank = jnp.searchsorted(jnp.asarray(table, jnp.int32), ticket, side="right")
    return jax.random.permutation(jax.random.fold_in(stream_key, 2), number_of)[rank].astype(jnp.int32)


def deal_out(stream_key, own, number, rows, number_of, top, bound, skew):
    ranking = jax.random.permutation(stream_key, number_of)
    heavy_load, common = portions_of(number_of, rows * top, bound, skew, True), portions_of(number_of, rows * top, bound, skew, False)
    places = jnp.arange(number_of)

    def named(tallies, turn):
        used = int((tallies > 0).sum())
        fixed = max(1, used // 4)
        shifted = fixed + (places - fixed + turn * (used - fixed)) % max(1, number_of - fixed)
        return jnp.zeros((number_of,), jnp.int32).at[ranking[jnp.where(places < fixed, places, shifted)]].set(jnp.asarray(tallies, jnp.int32))

    tallies = jnp.where(number % 4 == 0, named(heavy_load, number // 4), named(common, number - number // 4 - 1))
    mixed = jax.random.permutation(jax.random.fold_in(own, 3), number_of)
    giver, receiver = mixed[0:number_of // 2 * 2:2], mixed[1:number_of // 2 * 2:2]
    margin = jnp.minimum(tallies[giver] - 1, bound - tallies[receiver]) // 2
    margin = jnp.where((giver == ranking[0]) | (receiver == ranking[0]) | (tallies[receiver] == 0), 0, jnp.maximum(margin, 0))
    shifted = jax.random.randint(jax.random.fold_in(own, 4), (number_of // 2,), 0, 1 << 20) % (margin + 1)
    tallies = tallies.at[giver].add(-shifted).at[receiver].add(shifted)
    items = jnp.searchsorted(jnp.cumsum(tallies), jnp.arange(rows * top), side="right").astype(jnp.int32)
    listing = items.reshape(top, rows).T
    listing = listing[jax.random.permutation(jax.random.fold_in(own, 1), rows)]
    turn = jax.random.randint(jax.random.fold_in(own, 2), (rows, 1), 0, top)
    return jnp.take_along_axis(listing, (jnp.arange(top)[None, :] + turn) % top, axis=1)


def portions_of(amount, total, bound, slope, full):
    portions = [(1 << 20) // math.isqrt(grade ** slope) + 1 for grade in range(1, amount + 1)]
    largest = bound if full else min(bound, max(-(-total // amount), total * portions[0] // sum(portions)))
    least = 1 if total - largest >= amount - 1 else 0
    holding, spare = [largest] + [least] * (amount - 1), total - largest - least * (amount - 1)
    while spare > 0:
        candidates = [i for i in range(1, amount) if holding[i] < largest] or [i for i in range(1, amount) if holding[i] < bound]
        pool, remaining = sum([portions[i] for i in candidates]), spare
        for i in candidates:
            more = min(bound - holding[i], max(1, remaining * portions[i] // pool), spare)
            holding[i] = holding[i] + more
            spare = spare - more
    return np.array(holding)


def scatter_about(stream_key, dims, deviation, bound, pieces=(), held_as=jnp.bfloat16):
    gain = level_of(stream_key, dims, pieces, -0.22, 0.18) if pieces else 1.0
    drawn = jax.random.normal(stream_key, dims, jnp.float32) * deviation * gain
    return jnp.minimum(jnp.maximum(drawn, -bound), bound).astype(held_as)


def setup_inputs(seed: int = 0) -> dict:
    seeds = jax.random.split(jax.random.key(seed), 11)
    bag_lengths = set_ends(jax.random.randint(seeds[0], (TABLES, TOKENS), 1, BAG + 1), jax.random.fold_in(seeds[0], 1), 1, BAG).astype(jnp.int32)
    owners_keys = jax.random.split(jax.random.fold_in(seeds[1], 1), TABLES * TOKENS * BAG // (TOK_DEV * BAG))
    owners_turns = jax.random.permutation(jax.random.fold_in(seeds[1], 3), TABLES * TOKENS * BAG // (TOK_DEV * BAG))
    owners = jax.vmap(lambda own, number: deal_out(jax.random.fold_in(seeds[1], 2), own, number, TOK_DEV * BAG, N_DP, 1, CAP, 2))(owners_keys, owners_turns).reshape((TABLES, TOKENS, BAG, 1))
    row_slots = set_ends(skewed_ids(seeds[2], (TABLES, TOKENS, BAG), ROWS_DEV, 2), jax.random.fold_in(seeds[2], 3), 0, ROWS_DEV - 1).astype(jnp.int32)
    admit_mask = set_ends((jax.random.randint(seeds[3], (TABLES, TOKENS, BAG), 0, 4) < 3).astype(jnp.int32), jax.random.fold_in(seeds[3], 1), 0, 1)
    expired = set_ends((jax.random.randint(seeds[4], (TABLES, ROWS), 0, 8) < 1).astype(jnp.int32), jax.random.fold_in(seeds[4], 1), 0, 1)
    embeddings = scatter_about(seeds[5], (TABLES, ROWS, EMB), 0.5, 3.0, ((0, 2), (1, 16)), jnp.float32)
    accumulator = jnp.clip(jnp.exp(math.log(0.01) - 2.30258502 * jax.random.uniform(seeds[6], (TABLES, ROWS), jnp.float32) ** level_of(seeds[6], (TABLES, ROWS), ((0, 2), (1, 16)), -0.2, 0.2)), 0.001, 0.01)
    hidden_weight = scatter_about(seeds[7], (TABLES * EMB, HIDDEN_SIZE), (TABLES * EMB) ** -0.5, 0.125, ((1, 2),))
    output_weight = scatter_about(seeds[8], (HIDDEN_SIZE,), 0.15, 0.9, ((0, 2),), jnp.float32)
    labels = set_ends((jax.random.randint(seeds[9], (TOKENS,), 0, 2) < 1).astype(jnp.int32), jax.random.fold_in(seeds[9], 1), 0, 1)
    return {"bag_lengths": bag_lengths, "owners": owners, "row_slots": row_slots, "admit_mask": admit_mask, "expired": expired, "embeddings": embeddings, "accumulator": accumulator, "hidden_weight": hidden_weight, "output_weight": output_weight, "labels": labels}


LEARN_RATE = 0.05
ACC_RESET = 0.001

def silu_slope(preact):
    sig = jax.nn.sigmoid(preact)
    return sig * (1.0 + preact * (1.0 - sig))

def reference(bag_lengths, owners, row_slots, admit_mask, expired, embeddings, accumulator, hidden_weight, output_weight, labels):
    places = jnp.arange(BAG, dtype=jnp.int32)
    live_mask = ((places[None, None, :] < bag_lengths[:, :, None]) & (admit_mask == 1)).astype(jnp.float32)
    counted = lax.optimization_barrier(jnp.sum(live_mask, axis=2))
    bag_weight = live_mask / jnp.maximum(counted, 1.0)[:, :, None]
    global_rows = (owners[..., 0] * ROWS_DEV + row_slots).astype(jnp.int32)
    fresh_rows = jnp.where(expired[:, :, None] == 1, jnp.float32(0.0), embeddings)
    fresh_acc = jnp.where(expired == 1, jnp.float32(ACC_RESET), accumulator)

    def pool_table(inputs):
        table_rows, table_weight, table_index = inputs
        values = jnp.take(table_rows.astype(jnp.bfloat16), table_index, axis=0)
        return lax.optimization_barrier(jnp.sum(table_weight[:, :, None] * values.astype(jnp.float32), axis=1))
    pooled = lax.map(pool_table, (fresh_rows, bag_weight, global_rows))
    features = pooled.transpose(1, 0, 2).reshape(TOKENS, TABLES * EMB).astype(jnp.bfloat16)
    preact = jnp.dot(features, hidden_weight, preferred_element_type=jnp.float32)
    hidden = jax.nn.silu(preact).astype(jnp.bfloat16)
    logits = lax.optimization_barrier(jnp.sum(hidden.astype(jnp.float32) * output_weight, axis=1))
    dlogit = jax.nn.sigmoid(logits) - labels.astype(jnp.float32)
    dhidden = (dlogit[:, None] * output_weight * silu_slope(preact)).astype(jnp.bfloat16)
    weight_grad = lax.dot_general(features, dhidden, (((0,), (0,)), ((), ())), preferred_element_type=jnp.float32).astype(jnp.bfloat16)
    feature_grad = jnp.dot(dhidden, hidden_weight.T, preferred_element_type=jnp.float32)
    feature_grad = feature_grad.reshape(TOKENS, TABLES, EMB).transpose(1, 0, 2)

    def update_table(inputs):
        table_rows, table_acc, table_weight, table_index, table_grad = inputs
        lookup_grads = (table_weight[:, :, None] * table_grad[:, None, :]).astype(jnp.bfloat16)
        summed = jax.ops.segment_sum(lookup_grads.astype(jnp.float32).reshape(-1, EMB), table_index.reshape(-1), num_segments=ROWS)
        new_acc = table_acc + lax.optimization_barrier(jnp.mean(summed * summed, axis=1))
        new_rows = table_rows - LEARN_RATE * summed / jnp.sqrt(new_acc)[:, None]
        return (new_rows, new_acc)
    new_table, new_accum = lax.map(update_table, (fresh_rows, fresh_acc, bag_weight, global_rows, feature_grad))
    return (new_table, new_accum, weight_grad, logits)
```

```python
import functools

import jax
import jax.numpy as jnp
from jax import lax
from jax.experimental import pallas as pl
from jax.experimental.pallas import tpu as pltpu
from jax.sharding import PartitionSpec as P

LEARN_RATE = 0.05
ACC_RESET = 0.001
MESH = pl.DeviceIdType.MESH
BASE = 256


def silu_slope(preact):
    sig = jax.nn.sigmoid(preact)
    return sig * (1.0 + preact * (1.0 - sig))


def push_kernel(axis, groups, dims, *refs):
    count = len(dims)
    ins, outs = refs[:count], refs[count : 2 * count]
    send_sem, recv_sem, local_sem = refs[2 * count :]
    me = lax.axis_index(axis)

    def block(ref, dim, index):
        return ref.at[index] if dim == 0 else ref.at[:, index]

    barrier = pltpu.get_barrier_semaphore()

    def greet(step, carry):
        peer = lax.rem(me + step, groups)
        pl.semaphore_signal(barrier, inc=1, device_id={axis: peer}, device_id_type=MESH)
        return carry

    lax.fori_loop(1, groups, greet, 0)
    pl.semaphore_wait(barrier, groups - 1)

    for item in range(count):
        dim = dims[item]

        def send(step, carry, item=item, dim=dim):
            peer = lax.rem(me + step, groups)
            source = ins[item] if dim is None else block(ins[item], dim, peer)
            pltpu.make_async_remote_copy(
                src_ref=source,
                dst_ref=block(outs[item], dim or 0, me),
                send_sem=send_sem.at[item],
                recv_sem=recv_sem.at[item],
                device_id={axis: peer},
                device_id_type=MESH,
            ).start()
            return carry

        lax.fori_loop(1, groups, send, 0)
    kept = []
    for item in range(count):
        dim = dims[item]
        source = ins[item] if dim is None else block(ins[item], dim, me)
        kept.append(
            pltpu.make_async_copy(source, block(outs[item], dim or 0, me), local_sem.at[item])
        )
        kept[-1].start()
    for item in range(count):
        kept[item].wait()
        rest = block(outs[item], dims[item] or 0, pl.ds(0, groups - 1))
        pltpu.make_async_copy(rest, rest, recv_sem.at[item]).wait()
        pltpu.make_async_copy(rest, rest, send_sem.at[item]).wait()


def push(arrays, dims, axis, ident):
    groups = lax.axis_size(axis)
    shapes = [
        jax.ShapeDtypeStruct((groups,) + a.shape if d is None else a.shape, a.dtype)
        for a, d in zip(arrays, dims)
    ]
    count = len(arrays)
    return pl.pallas_call(
        functools.partial(push_kernel, axis, groups, tuple(dims)),
        out_shape=shapes,
        in_specs=[pl.BlockSpec(memory_space=pltpu.VMEM)] * count,
        out_specs=[pl.BlockSpec(memory_space=pltpu.VMEM)] * count,
        scratch_shapes=[
            pltpu.SemaphoreType.DMA((count,)),
            pltpu.SemaphoreType.DMA((count,)),
            pltpu.SemaphoreType.DMA((count,)),
        ],
        compiler_params=pltpu.CompilerParams(
            collective_id=ident, has_side_effects=True, vmem_limit_bytes=48 * 1024 * 1024
        ),
        name=f"push{ident}",
    )(*arrays)


def shards(
    bag_lengths,
    owners,
    row_slots,
    admit_mask,
    expired,
    embeddings,
    accumulator,
    hidden_weight,
    output_weight,
    labels,
):
    groups = lax.axis_size("dp")
    halves = lax.axis_size("mp")
    tab_dev, tok_dev, bag_size = row_slots.shape
    rows_dev = embeddings.shape[1]
    row_width = embeddings.shape[2]
    lookups = tok_dev * bag_size
    capacity = 2 * lookups // groups
    buffer_len = groups * capacity
    f32, bf16, i32 = jnp.float32, jnp.bfloat16, jnp.int32

    places = jnp.arange(bag_size, dtype=i32)
    live = (places[None, None, :] < bag_lengths[:, :, None]) & (admit_mask == 1)
    counted = jnp.sum(live.astype(f32), axis=2)
    scale = 1.0 / jnp.maximum(counted, 1.0)

    target = owners[..., 0].reshape(tab_dev, lookups)
    flat_slots = row_slots.reshape(tab_dev, lookups)
    lookup_ids = jnp.arange(lookups, dtype=i32)
    sample_of = jnp.where(live.reshape(tab_dev, lookups), lookup_ids[None] // bag_size + 1, 0)
    owner_hot = (target[:, None, :] == jnp.arange(groups, dtype=i32)[None, :, None]).astype(bf16)
    earlier = (lookup_ids[:, None] < lookup_ids[None, :]).astype(bf16)
    running = jnp.dot(
        owner_hot.reshape(tab_dev * groups, lookups), earlier, preferred_element_type=f32
    ).reshape(tab_dev, groups, lookups)
    ranked = jnp.sum(jnp.where(owner_hot > 0, running, 0.0), axis=1).astype(i32)
    rank_hot = (ranked[:, None, :] == jnp.arange(capacity, dtype=i32)[None, :, None]).astype(bf16)
    digits = jnp.stack(
        [flat_slots // BASE, flat_slots % BASE, sample_of // BASE, sample_of % BASE], axis=1
    ).astype(bf16)
    coded = (digits[:, :, None, :] * owner_hot[:, None, :, :]).reshape(
        tab_dev, 4 * groups, lookups
    )
    table_of = jnp.einsum("tal,tkl->tak", coded, rank_hot, preferred_element_type=f32).astype(i32)
    table_of = table_of.reshape(tab_dev, 4, groups, capacity)
    request = table_of[:, 0] * BASE + table_of[:, 1]
    slot_sample = (table_of[:, 2] * BASE + table_of[:, 3]).reshape(tab_dev, buffer_len)

    (arrived,) = push([request.transpose(1, 0, 2)], [0], "dp", 0)
    arrived = arrived.transpose(1, 0, 2).reshape(tab_dev, buffer_len)
    fresh_rows = jnp.where(expired[:, :, None] == 1, f32(0.0), embeddings)
    fresh_acc = jnp.where(expired == 1, f32(ACC_RESET), accumulator)
    row_pick = (arrived[:, :, None] == jnp.arange(rows_dev, dtype=i32)[None, None, :]).astype(bf16)
    fetched = jnp.einsum(
        "tbr,tre->tbe", row_pick, fresh_rows.astype(bf16), preferred_element_type=f32
    ).astype(bf16)
    (returned,) = push(
        [fetched.reshape(tab_dev, groups, capacity, row_width)], [1], "dp", 1
    )
    returned = returned.reshape(tab_dev, buffer_len, row_width)
    sample_ids = jnp.arange(1, tok_dev + 1, dtype=i32)
    pool = (slot_sample[:, None, :] == sample_ids[None, :, None]).astype(bf16)
    pooled = jnp.einsum("tnb,tbe->tne", pool, returned, preferred_element_type=f32)
    pooled = (pooled * scale[:, :, None]).astype(bf16)
    features = pooled.transpose(1, 0, 2).reshape(tok_dev, tab_dev * row_width)
    portion = lax.all_gather(features, "mp", axis=1, tiled=True)
    summed_pre = jnp.dot(portion, hidden_weight, preferred_element_type=f32)
    hidden = jax.nn.silu(summed_pre).astype(bf16)
    logits = lax.psum(jnp.sum(hidden.astype(f32) * output_weight, axis=1), "mp")
    dlogit = jax.nn.sigmoid(logits) - labels.astype(f32)
    dhidden = (dlogit[:, None] * output_weight * silu_slope(summed_pre)).astype(bf16)
    partial = lax.dot_general(
        dhidden, hidden_weight, (((1,), (1,)), ((), ())), preferred_element_type=f32
    ).astype(bf16)
    partial = partial.reshape(tok_dev, halves, tab_dev * row_width).transpose(1, 0, 2)
    (both,) = push([partial], [0], "mp", 2)
    feature_grad = jnp.sum(both.astype(f32), axis=0)
    per_table = feature_grad.reshape(tok_dev, tab_dev, row_width).transpose(1, 0, 2)
    per_table = (per_table * scale[:, :, None]).astype(bf16)
    sample_pick = (slot_sample[:, :, None] == sample_ids[None, None, :]).astype(bf16)
    outgoing = jnp.einsum(
        "tbn,tne->tbe", sample_pick, per_table, preferred_element_type=f32
    ).astype(bf16)
    share = portion.shape[1] // groups
    columns = portion.T.reshape(groups, share, tok_dev)
    grad_part, all_dhidden, all_columns = push(
        [outgoing.reshape(tab_dev, groups, capacity, row_width), dhidden, columns],
        [1, None, 0],
        "dp",
        3,
    )
    dense = jnp.einsum("gfn,gnh->fh", all_columns, all_dhidden, preferred_element_type=f32)
    (weight_grad,) = push([dense.astype(bf16)], [None], "dp", 4)
    weight_grad = weight_grad.reshape(portion.shape[1], dhidden.shape[1])
    selector = (arrived[:, None, :] == jnp.arange(rows_dev, dtype=i32)[None, :, None]).astype(bf16)
    summed = jnp.einsum(
        "trb,tbe->tre",
        selector,
        grad_part.reshape(tab_dev, buffer_len, row_width),
        preferred_element_type=f32,
    )
    new_acc = fresh_acc + jnp.mean(summed * summed, axis=2)
    new_rows = fresh_rows - LEARN_RATE * summed / jnp.sqrt(new_acc)[:, :, None]
    return (new_rows, new_acc, weight_grad, logits)


def solution(mesh):
    in_specs = (
        P("mp", "dp"),
        P("mp", "dp", None, None),
        P("mp", "dp", None),
        P("mp", "dp", None),
        P("mp", "dp"),
        P("mp", "dp", None),
        P("mp", "dp"),
        P(None, "mp"),
        P("mp"),
        P("dp"),
    )
    out_specs = (P("mp", "dp", None), P("mp", "dp"), P(None, "mp"), P("dp"))
    return jax.shard_map(shards, mesh=mesh, in_specs=in_specs, out_specs=out_specs, check_vma=False)
```

```python
import functools

import jax
import jax.numpy as jnp
from jax import lax
from jax.experimental import pallas as pl
from jax.experimental.pallas import tpu as pltpu
from jax.sharding import PartitionSpec as P

LEARN_RATE = 0.05
ACC_RESET = 0.001
MESH = pl.DeviceIdType.MESH
BASE = 256


def silu_slope(preact):
    sig = jax.nn.sigmoid(preact)
    return sig * (1.0 + preact * (1.0 - sig))


def push_kernel(axis, groups, dims, *refs):
    count = len(dims)
    ins, outs = refs[:count], refs[count : 2 * count]
    send_sem, recv_sem, local_sem = refs[2 * count :]
    me = lax.axis_index(axis)

    def block(ref, dim, index):
        return ref.at[index] if dim == 0 else ref.at[:, index]

    barrier = pltpu.get_barrier_semaphore()

    def greet(step, carry):
        peer = lax.rem(me + step, groups)
        pl.semaphore_signal(barrier, inc=1, device_id={axis: peer}, device_id_type=MESH)
        return carry

    lax.fori_loop(1, groups, greet, 0)
    pl.semaphore_wait(barrier, groups - 1)

    for item in range(count):
        dim = dims[item]

        def send(step, carry, item=item, dim=dim):
            peer = lax.rem(me + step, groups)
            source = ins[item] if dim is None else block(ins[item], dim, peer)
            pltpu.make_async_remote_copy(
                src_ref=source,
                dst_ref=block(outs[item], dim or 0, me),
                send_sem=send_sem.at[item],
                recv_sem=recv_sem.at[item],
                device_id={axis: peer},
                device_id_type=MESH,
            ).start()
            return carry

        lax.fori_loop(1, groups, send, 0)
    kept = []
    for item in range(count):
        dim = dims[item]
        source = ins[item] if dim is None else block(ins[item], dim, me)
        kept.append(
            pltpu.make_async_copy(source, block(outs[item], dim or 0, me), local_sem.at[item])
        )
        kept[-1].start()
    for item in range(count):
        kept[item].wait()
        rest = block(outs[item], dims[item] or 0, pl.ds(0, groups - 1))
        pltpu.make_async_copy(rest, rest, recv_sem.at[item]).wait()
        pltpu.make_async_copy(rest, rest, send_sem.at[item]).wait()


def push(arrays, dims, axis, ident):
    groups = lax.axis_size(axis)
    shapes = [
        jax.ShapeDtypeStruct((groups,) + a.shape if d is None else a.shape, a.dtype)
        for a, d in zip(arrays, dims)
    ]
    count = len(arrays)
    return pl.pallas_call(
        functools.partial(push_kernel, axis, groups, tuple(dims)),
        out_shape=shapes,
        in_specs=[pl.BlockSpec(memory_space=pltpu.VMEM)] * count,
        out_specs=[pl.BlockSpec(memory_space=pltpu.VMEM)] * count,
        scratch_shapes=[
            pltpu.SemaphoreType.DMA((count,)),
            pltpu.SemaphoreType.DMA((count,)),
            pltpu.SemaphoreType.DMA((count,)),
        ],
        compiler_params=pltpu.CompilerParams(
            collective_id=ident, has_side_effects=True, vmem_limit_bytes=48 * 1024 * 1024
        ),
        name=f"push{ident}",
    )(*arrays)


def grid_of(groups):
    chips = groups // 2
    inner = 1
    while inner * inner * 4 <= chips and chips % (inner * 2) == 0:
        inner *= 2
    return chips // inner, inner


def gather_kernel(axis, groups, count, *refs):
    ins, outs = refs[:count], refs[count : 2 * count]
    send_sem, outer_sem, inner_sem, core_sem, local_sem = refs[2 * count :]
    outer, inner = grid_of(groups)
    me = lax.axis_index(axis)
    core = lax.rem(me, 2)
    row = lax.rem(lax.div(me, 2), inner)
    plane = lax.div(me, 2 * inner)
    partner = me + 1 - 2 * core

    def device(p, r):
        return (p * inner + r) * 2 + core

    def plane_peer(step):
        return device(lax.rem(plane + step, outer), row)

    def row_peer(step):
        return device(plane, lax.rem(row + step, inner))

    def source(up, across):
        return device(lax.rem(plane + outer - up, outer), lax.rem(row + inner - across, inner))

    barrier = pltpu.get_barrier_semaphore()

    def greet(peer):
        pl.semaphore_signal(barrier, inc=1, device_id={axis: peer}, device_id_type=MESH)

    def loop(low, high, body):
        def step(index, carry):
            body(index)
            return carry

        lax.fori_loop(low, high, step, 0)

    loop(1, outer, lambda step: greet(plane_peer(step)))
    loop(1, inner, lambda step: greet(row_peer(step)))
    greet(partner)
    pl.semaphore_wait(barrier, outer + inner - 1)

    def send(item, src, owner, sem, peer):
        pltpu.make_async_remote_copy(
            src_ref=src,
            dst_ref=outs[item].at[owner],
            send_sem=send_sem.at[item],
            recv_sem=sem,
            device_id={axis: peer},
            device_id_type=MESH,
        ).start()

    def spread(item, src, owner, up):
        loop(
            1,
            inner,
            lambda step: send(item, src, owner, inner_sem.at[item, up, step], row_peer(step)),
        )
        send(item, src, owner, core_sem.at[item], partner)

    def arrive(item, owner, sem):
        pltpu.make_async_copy(outs[item].at[owner], outs[item].at[owner], sem).wait()

    for item in range(count):
        loop(
            1,
            outer,
            lambda step: send(item, ins[item], me, outer_sem.at[item, step], plane_peer(step)),
        )
        spread(item, ins[item], me, 0)
    kept = []
    for item in range(count):
        kept.append(pltpu.make_async_copy(ins[item], outs[item].at[me], local_sem.at[item]))
        kept[-1].start()

    def from_plane(item, up):
        owner = source(up, 0)
        arrive(item, owner, outer_sem.at[item, up])
        spread(item, outs[item].at[owner], owner, up)

    def from_row(item, up, across):
        owner = source(up, across)
        arrive(item, owner, inner_sem.at[item, up, across])
        send(item, outs[item].at[owner], owner, core_sem.at[item], partner)

    for item in range(count):
        loop(1, outer, lambda up: from_plane(item, up))
    for item in range(count):
        loop(0, outer, lambda up: loop(1, inner, lambda across: from_row(item, up, across)))
    for item in range(count):
        kept[item].wait()
        part = outs[item].at[pl.ds(0, outer * inner)]
        pltpu.make_async_copy(part, part, core_sem.at[item]).wait()
        rest = outs[item].at[pl.ds(0, groups - 1)]
        pltpu.make_async_copy(rest, rest, send_sem.at[item]).wait()


def gather(arrays, axis, ident):
    groups = lax.axis_size(axis)
    outer, inner = grid_of(groups)
    count = len(arrays)
    return pl.pallas_call(
        functools.partial(gather_kernel, axis, groups, count),
        out_shape=[jax.ShapeDtypeStruct((groups,) + a.shape, a.dtype) for a in arrays],
        in_specs=[pl.BlockSpec(memory_space=pltpu.VMEM)] * count,
        out_specs=[pl.BlockSpec(memory_space=pltpu.VMEM)] * count,
        scratch_shapes=[
            pltpu.SemaphoreType.DMA((count,)),
            pltpu.SemaphoreType.DMA((count, outer)),
            pltpu.SemaphoreType.DMA((count, outer, inner)),
            pltpu.SemaphoreType.DMA((count,)),
            pltpu.SemaphoreType.DMA((count,)),
        ],
        compiler_params=pltpu.CompilerParams(
            collective_id=ident, has_side_effects=True, vmem_limit_bytes=48 * 1024 * 1024
        ),
        name=f"gather{ident}",
    )(*arrays)


def shards(
    bag_lengths,
    owners,
    row_slots,
    admit_mask,
    expired,
    embeddings,
    accumulator,
    hidden_weight,
    output_weight,
    labels,
):
    groups = lax.axis_size("dp")
    halves = lax.axis_size("mp")
    tab_dev, tok_dev, bag_size = row_slots.shape
    rows_dev = embeddings.shape[1]
    row_width = embeddings.shape[2]
    lookups = tok_dev * bag_size
    capacity = 2 * lookups // groups
    buffer_len = groups * capacity
    f32, bf16, i32 = jnp.float32, jnp.bfloat16, jnp.int32

    places = jnp.arange(bag_size, dtype=i32)
    live = (places[None, None, :] < bag_lengths[:, :, None]) & (admit_mask == 1)
    counted = jnp.sum(live.astype(f32), axis=2)
    scale = 1.0 / jnp.maximum(counted, 1.0)

    target = owners[..., 0].reshape(tab_dev, lookups)
    flat_slots = row_slots.reshape(tab_dev, lookups)
    lookup_ids = jnp.arange(lookups, dtype=i32)
    sample_of = jnp.where(live.reshape(tab_dev, lookups), lookup_ids[None] // bag_size + 1, 0)
    owner_hot = (target[:, None, :] == jnp.arange(groups, dtype=i32)[None, :, None]).astype(bf16)
    earlier = (lookup_ids[:, None] < lookup_ids[None, :]).astype(bf16)
    running = jnp.dot(
        owner_hot.reshape(tab_dev * groups, lookups), earlier, preferred_element_type=f32
    ).reshape(tab_dev, groups, lookups)
    ranked = jnp.sum(jnp.where(owner_hot > 0, running, 0.0), axis=1).astype(i32)
    rank_hot = (ranked[:, None, :] == jnp.arange(capacity, dtype=i32)[None, :, None]).astype(bf16)
    digits = jnp.stack(
        [flat_slots // BASE, flat_slots % BASE, sample_of // BASE, sample_of % BASE], axis=1
    ).astype(bf16)
    coded = (digits[:, :, None, :] * owner_hot[:, None, :, :]).reshape(
        tab_dev, 4 * groups, lookups
    )
    table_of = jnp.einsum("tal,tkl->tak", coded, rank_hot, preferred_element_type=f32).astype(i32)
    table_of = table_of.reshape(tab_dev, 4, groups, capacity)
    request = table_of[:, 0] * BASE + table_of[:, 1]
    slot_sample = (table_of[:, 2] * BASE + table_of[:, 3]).reshape(tab_dev, buffer_len)

    packed = request * (tok_dev + 1) + slot_sample.reshape(tab_dev, groups, capacity)
    (arrived,) = push([packed.transpose(1, 0, 2)], [0], "dp", 0)
    arrived = arrived.transpose(1, 0, 2)
    came_from = arrived % (tok_dev + 1)
    arrived = (arrived // (tok_dev + 1)).reshape(tab_dev, buffer_len)
    fresh_rows = jnp.where(expired[:, :, None] == 1, f32(0.0), embeddings)
    fresh_acc = jnp.where(expired == 1, f32(ACC_RESET), accumulator)
    row_pick = (arrived[:, :, None] == jnp.arange(rows_dev, dtype=i32)[None, None, :]).astype(bf16)
    fetched = jnp.einsum(
        "tbr,tre->tbe", row_pick, fresh_rows.astype(bf16), preferred_element_type=f32
    ).astype(bf16)
    (returned,) = push(
        [fetched.reshape(tab_dev, groups, capacity, row_width)], [1], "dp", 1
    )
    returned = returned.reshape(tab_dev, buffer_len, row_width)
    sample_ids = jnp.arange(1, tok_dev + 1, dtype=i32)
    pool = (slot_sample[:, None, :] == sample_ids[None, :, None]).astype(bf16)
    pooled = jnp.einsum("tnb,tbe->tne", pool, returned, preferred_element_type=f32)
    pooled = (pooled * scale[:, :, None]).astype(bf16)
    features = pooled.transpose(1, 0, 2).reshape(tok_dev, tab_dev * row_width)
    portion = lax.all_gather(features, "mp", axis=1, tiled=True)
    summed_pre = jnp.dot(portion, hidden_weight, preferred_element_type=f32)
    hidden = jax.nn.silu(summed_pre).astype(bf16)
    logits = lax.psum(jnp.sum(hidden.astype(f32) * output_weight, axis=1), "mp")
    dlogit = jax.nn.sigmoid(logits) - labels.astype(f32)
    dhidden = (dlogit[:, None] * output_weight * silu_slope(summed_pre)).astype(bf16)
    partial = lax.dot_general(
        dhidden, hidden_weight, (((1,), (1,)), ((), ())), preferred_element_type=f32
    ).astype(bf16)
    partial = partial.reshape(tok_dev, halves, tab_dev * row_width).transpose(1, 0, 2)
    (both,) = push([partial], [0], "mp", 2)
    feature_grad = jnp.sum(both.astype(f32), axis=0)
    per_table = feature_grad.reshape(tok_dev, tab_dev, row_width).transpose(1, 0, 2)
    per_table = (per_table * scale[:, :, None]).astype(bf16)
    share = portion.shape[1] // groups
    columns = portion.T.reshape(groups, share, tok_dev)
    (all_columns,) = push([columns], [0], "dp", 3)
    all_dhidden, all_grads = gather([dhidden, per_table], "dp", 5)
    sample_pick = (came_from[..., None] == sample_ids).astype(bf16)
    grad_part = jnp.einsum(
        "tgkn,gtne->tgke", sample_pick, all_grads, preferred_element_type=f32
    ).astype(bf16)
    dense = jnp.einsum("gfn,gnh->fh", all_columns, all_dhidden, preferred_element_type=f32)
    (weight_grad,) = gather([dense.astype(bf16)], "dp", 4)
    weight_grad = weight_grad.reshape(portion.shape[1], dhidden.shape[1])
    selector = (arrived[:, None, :] == jnp.arange(rows_dev, dtype=i32)[None, :, None]).astype(bf16)
    summed = jnp.einsum(
        "trb,tbe->tre",
        selector,
        grad_part.reshape(tab_dev, buffer_len, row_width),
        preferred_element_type=f32,
    )
    new_acc = fresh_acc + jnp.mean(summed * summed, axis=2)
    new_rows = fresh_rows - LEARN_RATE * summed / jnp.sqrt(new_acc)[:, :, None]
    return (new_rows, new_acc, weight_grad, logits)


def solution(mesh):
    in_specs = (
        P("mp", "dp"),
        P("mp", "dp", None, None),
        P("mp", "dp", None),
        P("mp", "dp", None),
        P("mp", "dp"),
        P("mp", "dp", None),
        P("mp", "dp"),
        P(None, "mp"),
        P("mp"),
        P("dp"),
    )
    out_specs = (P("mp", "dp", None), P("mp", "dp"), P(None, "mp"), P("dp"))
    return jax.shard_map(shards, mesh=mesh, in_specs=in_specs, out_specs=out_specs, check_vma=False)
```

```python
import functools

import jax
import jax.numpy as jnp
from jax import lax
from jax.experimental import pallas as pl
from jax.experimental.pallas import tpu as pltpu
from jax.sharding import PartitionSpec as P

LEARN_RATE = 0.05
ACC_RESET = 0.001
MESH = pl.DeviceIdType.MESH
BASE = 256


def silu_slope(preact):
    sig = jax.nn.sigmoid(preact)
    return sig * (1.0 + preact * (1.0 - sig))


def push_kernel(axis, groups, dims, *refs):
    count = len(dims)
    ins, outs = refs[:count], refs[count : 2 * count]
    send_sem, recv_sem, local_sem = refs[2 * count :]
    me = lax.axis_index(axis)

    def block(ref, dim, index):
        return ref.at[index] if dim == 0 else ref.at[:, index]

    barrier = pltpu.get_barrier_semaphore()

    def greet(step, carry):
        peer = lax.rem(me + step, groups)
        pl.semaphore_signal(barrier, inc=1, device_id={axis: peer}, device_id_type=MESH)
        return carry

    lax.fori_loop(1, groups, greet, 0)
    pl.semaphore_wait(barrier, groups - 1)

    for item in range(count):
        dim = dims[item]

        def send(turn, carry, item=item, dim=dim):
            half, odd = lax.div(turn + 1, 2), lax.rem(turn, 2)
            peer = lax.rem(me + odd * half + (1 - odd) * (groups - half), groups)
            source = ins[item] if dim is None else block(ins[item], dim, peer)
            pltpu.make_async_remote_copy(
                src_ref=source,
                dst_ref=block(outs[item], dim or 0, me),
                send_sem=send_sem.at[item],
                recv_sem=recv_sem.at[item],
                device_id={axis: peer},
                device_id_type=MESH,
            ).start()
            return carry

        lax.fori_loop(1, groups, send, 0)
    kept = []
    for item in range(count):
        dim = dims[item]
        source = ins[item] if dim is None else block(ins[item], dim, me)
        kept.append(
            pltpu.make_async_copy(source, block(outs[item], dim or 0, me), local_sem.at[item])
        )
        kept[-1].start()
    for item in range(count):
        kept[item].wait()
        rest = block(outs[item], dims[item] or 0, pl.ds(0, groups - 1))
        pltpu.make_async_copy(rest, rest, recv_sem.at[item]).wait()
        pltpu.make_async_copy(rest, rest, send_sem.at[item]).wait()


def push(arrays, dims, axis, ident):
    groups = lax.axis_size(axis)
    shapes = [
        jax.ShapeDtypeStruct((groups,) + a.shape if d is None else a.shape, a.dtype)
        for a, d in zip(arrays, dims)
    ]
    count = len(arrays)
    return pl.pallas_call(
        functools.partial(push_kernel, axis, groups, tuple(dims)),
        out_shape=shapes,
        in_specs=[pl.BlockSpec(memory_space=pltpu.VMEM)] * count,
        out_specs=[pl.BlockSpec(memory_space=pltpu.VMEM)] * count,
        scratch_shapes=[
            pltpu.SemaphoreType.DMA((count,)),
            pltpu.SemaphoreType.DMA((count,)),
            pltpu.SemaphoreType.DMA((count,)),
        ],
        compiler_params=pltpu.CompilerParams(
            collective_id=ident, has_side_effects=True, vmem_limit_bytes=48 * 1024 * 1024
        ),
        name=f"push{ident}",
    )(*arrays)


def grid_of(groups):
    chips = groups // 2
    inner = 1
    while inner * inner * 4 <= chips and chips % (inner * 2) == 0:
        inner *= 2
    return chips // inner, inner


def gather_kernel(axis, groups, count, *refs):
    ins, outs = refs[:count], refs[count : 2 * count]
    send_sem, outer_sem, inner_sem, core_sem, local_sem = refs[2 * count :]
    outer, inner = grid_of(groups)
    me = lax.axis_index(axis)
    core = lax.rem(me, 2)
    row = lax.rem(lax.div(me, 2), inner)
    plane = lax.div(me, 2 * inner)
    partner = me + 1 - 2 * core

    def device(p, r):
        return (p * inner + r) * 2 + core

    def plane_peer(step):
        return device(lax.rem(plane + step, outer), row)

    def row_peer(step):
        return device(plane, lax.rem(row + step, inner))

    def source(up, across):
        return device(lax.rem(plane + outer - up, outer), lax.rem(row + inner - across, inner))

    barrier = pltpu.get_barrier_semaphore()

    def greet(peer):
        pl.semaphore_signal(barrier, inc=1, device_id={axis: peer}, device_id_type=MESH)

    def loop(low, high, body):
        def step(index, carry):
            body(index)
            return carry

        lax.fori_loop(low, high, step, 0)

    loop(1, outer, lambda step: greet(plane_peer(step)))
    loop(1, inner, lambda step: greet(row_peer(step)))
    greet(partner)
    pl.semaphore_wait(barrier, outer + inner - 1)

    def send(item, src, owner, sem, peer):
        pltpu.make_async_remote_copy(
            src_ref=src,
            dst_ref=outs[item].at[owner],
            send_sem=send_sem.at[item],
            recv_sem=sem,
            device_id={axis: peer},
            device_id_type=MESH,
        ).start()

    def spread(item, src, owner, up):
        loop(
            1,
            inner,
            lambda step: send(item, src, owner, inner_sem.at[item, up, step], row_peer(step)),
        )
        send(item, src, owner, core_sem.at[item], partner)

    def arrive(item, owner, sem):
        pltpu.make_async_copy(outs[item].at[owner], outs[item].at[owner], sem).wait()

    for item in range(count):
        loop(
            1,
            outer,
            lambda step: send(item, ins[item], me, outer_sem.at[item, step], plane_peer(step)),
        )
        spread(item, ins[item], me, 0)
    kept = []
    for item in range(count):
        kept.append(pltpu.make_async_copy(ins[item], outs[item].at[me], local_sem.at[item]))
        kept[-1].start()

    def from_plane(item, up):
        owner = source(up, 0)
        arrive(item, owner, outer_sem.at[item, up])
        spread(item, outs[item].at[owner], owner, up)

    def from_row(item, up, across):
        owner = source(up, across)
        arrive(item, owner, inner_sem.at[item, up, across])
        send(item, outs[item].at[owner], owner, core_sem.at[item], partner)

    for item in range(count):
        loop(1, outer, lambda up: from_plane(item, up))
    for item in range(count):
        loop(0, outer, lambda up: loop(1, inner, lambda across: from_row(item, up, across)))
    for item in range(count):
        kept[item].wait()
        part = outs[item].at[pl.ds(0, outer * inner)]
        pltpu.make_async_copy(part, part, core_sem.at[item]).wait()
        rest = outs[item].at[pl.ds(0, groups - 1)]
        pltpu.make_async_copy(rest, rest, send_sem.at[item]).wait()


def gather(arrays, axis, ident):
    groups = lax.axis_size(axis)
    outer, inner = grid_of(groups)
    count = len(arrays)
    return pl.pallas_call(
        functools.partial(gather_kernel, axis, groups, count),
        out_shape=[jax.ShapeDtypeStruct((groups,) + a.shape, a.dtype) for a in arrays],
        in_specs=[pl.BlockSpec(memory_space=pltpu.VMEM)] * count,
        out_specs=[pl.BlockSpec(memory_space=pltpu.VMEM)] * count,
        scratch_shapes=[
            pltpu.SemaphoreType.DMA((count,)),
            pltpu.SemaphoreType.DMA((count, outer)),
            pltpu.SemaphoreType.DMA((count, outer, inner)),
            pltpu.SemaphoreType.DMA((count,)),
            pltpu.SemaphoreType.DMA((count,)),
        ],
        compiler_params=pltpu.CompilerParams(
            collective_id=ident, has_side_effects=True, vmem_limit_bytes=48 * 1024 * 1024
        ),
        name=f"gather{ident}",
    )(*arrays)


def shards(
    bag_lengths,
    owners,
    row_slots,
    admit_mask,
    expired,
    embeddings,
    accumulator,
    hidden_weight,
    output_weight,
    labels,
):
    groups = lax.axis_size("dp")
    halves = lax.axis_size("mp")
    tab_dev, tok_dev, bag_size = row_slots.shape
    rows_dev = embeddings.shape[1]
    row_width = embeddings.shape[2]
    lookups = tok_dev * bag_size
    capacity = 2 * lookups // groups
    buffer_len = groups * capacity
    f32, bf16, i32 = jnp.float32, jnp.bfloat16, jnp.int32

    places = jnp.arange(bag_size, dtype=i32)
    live = (places[None, None, :] < bag_lengths[:, :, None]) & (admit_mask == 1)
    counted = jnp.sum(live.astype(f32), axis=2)
    scale = 1.0 / jnp.maximum(counted, 1.0)

    target = owners[..., 0].reshape(tab_dev, lookups)
    flat_slots = row_slots.reshape(tab_dev, lookups)
    lookup_ids = jnp.arange(lookups, dtype=i32)
    sample_of = jnp.where(live.reshape(tab_dev, lookups), lookup_ids[None] // bag_size + 1, 0)
    owner_hot = (target[:, None, :] == jnp.arange(groups, dtype=i32)[None, :, None]).astype(bf16)
    earlier = (lookup_ids[:, None] < lookup_ids[None, :]).astype(bf16)
    running = jnp.dot(
        owner_hot.reshape(tab_dev * groups, lookups), earlier, preferred_element_type=f32
    ).reshape(tab_dev, groups, lookups)
    ranked = jnp.sum(jnp.where(owner_hot > 0, running, 0.0), axis=1).astype(i32)
    rank_hot = (ranked[:, None, :] == jnp.arange(capacity, dtype=i32)[None, :, None]).astype(bf16)
    digits = jnp.stack(
        [flat_slots // BASE, flat_slots % BASE, sample_of // BASE, sample_of % BASE], axis=1
    ).astype(bf16)
    coded = (digits[:, :, None, :] * owner_hot[:, None, :, :]).reshape(
        tab_dev, 4 * groups, lookups
    )
    table_of = jnp.einsum("tal,tkl->tak", coded, rank_hot, preferred_element_type=f32).astype(i32)
    table_of = table_of.reshape(tab_dev, 4, groups, capacity)
    request = table_of[:, 0] * BASE + table_of[:, 1]
    slot_sample = (table_of[:, 2] * BASE + table_of[:, 3]).reshape(tab_dev, buffer_len)

    packed = request * (tok_dev + 1) + slot_sample.reshape(tab_dev, groups, capacity)
    (arrived,) = push([packed.transpose(1, 0, 2)], [0], "dp", 0)
    arrived = arrived.transpose(1, 0, 2)
    came_from = arrived % (tok_dev + 1)
    arrived = (arrived // (tok_dev + 1)).reshape(tab_dev, buffer_len)
    fresh_rows = jnp.where(expired[:, :, None] == 1, f32(0.0), embeddings)
    fresh_acc = jnp.where(expired == 1, f32(ACC_RESET), accumulator)
    row_pick = (arrived[:, :, None] == jnp.arange(rows_dev, dtype=i32)[None, None, :]).astype(bf16)
    fetched = jnp.einsum(
        "tbr,tre->tbe", row_pick, fresh_rows.astype(bf16), preferred_element_type=f32
    ).astype(bf16)
    (returned,) = push(
        [fetched.reshape(tab_dev, groups, capacity, row_width)], [1], "dp", 1
    )
    returned = returned.reshape(tab_dev, buffer_len, row_width)
    sample_ids = jnp.arange(1, tok_dev + 1, dtype=i32)
    pool = (slot_sample[:, None, :] == sample_ids[None, :, None]).astype(bf16)
    pooled = jnp.einsum("tnb,tbe->tne", pool, returned, preferred_element_type=f32)
    pooled = (pooled * scale[:, :, None]).astype(bf16)
    features = pooled.transpose(1, 0, 2).reshape(tok_dev, tab_dev * row_width)
    portion = lax.all_gather(features, "mp", axis=1, tiled=True)
    summed_pre = jnp.dot(portion, hidden_weight, preferred_element_type=f32)
    hidden = jax.nn.silu(summed_pre).astype(bf16)
    logits = lax.psum(jnp.sum(hidden.astype(f32) * output_weight, axis=1), "mp")
    dlogit = jax.nn.sigmoid(logits) - labels.astype(f32)
    dhidden = (dlogit[:, None] * output_weight * silu_slope(summed_pre)).astype(bf16)
    partial = lax.dot_general(
        dhidden, hidden_weight, (((1,), (1,)), ((), ())), preferred_element_type=f32
    ).astype(bf16)
    partial = partial.reshape(tok_dev, halves, tab_dev * row_width).transpose(1, 0, 2)
    (both,) = push([partial], [0], "mp", 2)
    feature_grad = jnp.sum(both.astype(f32), axis=0)
    per_table = feature_grad.reshape(tok_dev, tab_dev, row_width).transpose(1, 0, 2)
    per_table = (per_table * scale[:, :, None]).astype(bf16)
    share = portion.shape[1] // groups
    columns = portion.T.reshape(groups, share, tok_dev)
    all_columns = lax.all_to_all(columns, "dp", split_axis=0, concat_axis=0, tiled=True)
    all_dhidden, all_grads = gather([dhidden, per_table], "dp", 5)
    sample_pick = (came_from[..., None] == sample_ids).astype(bf16)
    grad_part = jnp.einsum(
        "tgkn,gtne->tgke", sample_pick, all_grads, preferred_element_type=f32
    ).astype(bf16)
    dense = jnp.einsum("gfn,gnh->fh", all_columns, all_dhidden, preferred_element_type=f32)
    (weight_grad,) = gather([dense.astype(bf16)], "dp", 4)
    weight_grad = weight_grad.reshape(portion.shape[1], dhidden.shape[1])
    selector = (arrived[:, None, :] == jnp.arange(rows_dev, dtype=i32)[None, :, None]).astype(bf16)
    summed = jnp.einsum(
        "trb,tbe->tre",
        selector,
        grad_part.reshape(tab_dev, buffer_len, row_width),
        preferred_element_type=f32,
    )
    new_acc = fresh_acc + jnp.mean(summed * summed, axis=2)
    new_rows = fresh_rows - LEARN_RATE * summed / jnp.sqrt(new_acc)[:, :, None]
    return (new_rows, new_acc, weight_grad, logits)


def solution(mesh):
    in_specs = (
        P("mp", "dp"),
        P("mp", "dp", None, None),
        P("mp", "dp", None),
        P("mp", "dp", None),
        P("mp", "dp"),
        P("mp", "dp", None),
        P("mp", "dp"),
        P(None, "mp"),
        P("mp"),
        P("dp"),
    )
    out_specs = (P("mp", "dp", None), P("mp", "dp"), P(None, "mp"), P("dp"))
    return jax.shard_map(shards, mesh=mesh, in_specs=in_specs, out_specs=out_specs, check_vma=False)
```
